256 devices in a mesh: dp: 16 (over x, y_hi, core), ctx: 16 (over y_lo, z).
Axes of the slice: x: 4, y: 4 (y_hi: 2, y_lo: 2; y = y_hi * 2 + y_lo), z: 8, core: 2. Of those that a mesh axis runs over, the one named last changes fastest.
Arguments:
- normed: bfloat16 [16, 2048, 5376], P('dp', 'ctx'), may hold values from -6 to 6
- queries: bfloat16 [16, 2048, 2048], P('dp', 'ctx'), may hold values from -8 to 8
- keys: bfloat16 [16, 2048, 1024], P('dp', 'ctx'), may hold values from -8 to 8
- values: bfloat16 [16, 2048, 1024], P('dp', 'ctx'), may hold values from -6 to 6
- out_grad: bfloat16 [16, 2048, 2048], P('dp', 'ctx'), may hold values from -150 to 150
- segment_ids: int32 [16, 2048], P('dp'), may hold values from 0 to 3, never falling along the last dimension, each value on 1 to 1536 neighbouring positions
Outputs:
- grad_queries: bfloat16 [16, 2048, 2048], P('dp', 'ctx')
- grad_keys: bfloat16 [16, 2048, 1024], P('dp', 'ctx')
- grad_values: bfloat16 [16, 2048, 1024], P('dp', 'ctx')
- grad_weight: bfloat16 [5376, 1024], P('ctx', 'dp')
The draws below stay inside these ranges and needn't reach their ends.
Inputs may be any that keep to these rules, and one draw needn't show every extreme that they name: `segment_ids`: within a sequence the document numbers never fall, and a document has at most 1536 positions.
All inputs are finite; a program needn't handle non-finite values.
Results may differ from the reference program's by a relative error of at most 0.022.
Values may be sent and summed in bfloat16 or wider, within the bound.
No kernel may reach another device: no remote copies, remote signals or barrier semaphores. Data moves between devices by JAX's collectives and lax.ppermute only.
A program may use at most 128 MiB of HBM per device.

```python
import math
import jax
import jax.numpy as jnp
import numpy as np
from jax import lax

D = 5376
QUERY_HEADS = 16
KEY_VALUE_HEADS = 8
HEAD_SIZE = 128
WINDOW = 1024
DOCS = 4
TOK_DEV = 128
SEQUENCE_COUNT = 16
SEQUENCE_LENGTH = 2048
ALL_TOK = 32768
N_CTX = 16


def draw_queries(key, part):
    sampled_values = jax.random.normal(jax.random.fold_in(key, 11), (SEQUENCE_COUNT, SEQUENCE_LENGTH, QUERY_HEADS * HEAD_SIZE), jnp.float32)
    return jnp.clip(sampled_values, -8.0, 8.0).astype(jnp.bfloat16)


def draw_keys(key, part):
    sampled_values = jax.random.normal(jax.random.fold_in(key, 13), (SEQUENCE_COUNT, SEQUENCE_LENGTH, KEY_VALUE_HEADS * HEAD_SIZE), jnp.float32)
    return jnp.clip(sampled_values, -8.0, 8.0).astype(jnp.bfloat16)


def with_spikes(array, key, source, target, parts, factor):
    owner, partner = [(jnp.arange(array.shape[position]) // (array.shape[position] // parts)).reshape([-1 if axis == position else 1 for axis in range(array.ndim)]) for position in (source, target)]
    chosen = jax.random.permutation(key, parts)[partner]
    strong = (owner == chosen) | (owner == (partner + parts // 2) % parts)
    return jnp.where(strong, factor * array, array)


def steps_of(rng, extent, cuts, low, top_value):
    def one(axis_at, blocks):
        steps = jax.random.uniform(jax.random.fold_in(jax.random.fold_in(rng, 6), axis_at), (blocks,), jnp.float32, low / len(cuts), top_value / len(cuts))
        return jnp.repeat(jnp.exp(steps), extent[axis_at] // blocks).reshape((-1,) + (1,) * (len(extent) - axis_at - 1))

    loudness = one(*cuts[0])
    for cut in cuts[1:]:
        loudness = loudness * one(*cut)
    return loudness


def profile(number_of, total, limit, slope):
    loads = [(1 << 20) // math.isqrt(standing ** slope) + 1 for standing in range(2, number_of + 1)]
    surplus, given = total - limit - (number_of - 1), [1] * (number_of - 1)
    while surplus > 0:
        candidates = [i for i in range(number_of - 1) if given[i] < limit]
        mass, left = sum([loads[i] for i in candidates]), surplus
        for i in candidates:
            addition = min(limit - given[i], max(1, left * loads[i] // mass), surplus)
            given[i] = given[i] + addition
            surplus = surplus - addition
    return np.array([limit] + given)


def uneven_parts(own_key, count, total, reach, lean):
    if count == 2:
        one = jax.random.randint(own_key, (), max(1, total - reach), min(reach, total - 1) + 1)
        return jnp.stack([one, total - one])
    tallies = jnp.asarray(profile(count, total, reach, lean), jnp.int32)
    twos = (count - 1) // 2
    donor, taker = tallies[1:1 + 2 * twos:2], tallies[2:2 + 2 * twos:2]
    room = jnp.minimum(donor - 1, reach - taker)
    shifted = jax.random.randint(jax.random.fold_in(own_key, 1), (twos,), 0, 1 << 20) % (room + 1)
    tallies = tallies.at[1:1 + 2 * twos:2].set(donor - shifted).at[2:2 + 2 * twos:2].set(taker + shifted)
    return tallies[jax.random.permutation(jax.random.fold_in(own_key, 2), count)]


def gaussian(stream_key, dims, spread, limit, cuts=(), held_as=jnp.bfloat16):
    values = jax.random.normal(stream_key, dims, jnp.float32) * spread
    if len(cuts) > 0:
        values = steps_of(stream_key, dims, cuts, -0.22, 0.18) * values
    return jnp.clip(values, min=-limit, max=limit).astype(held_as)


def noise_with(key, extent, scale, reach, shards, heavy, held_as=jnp.bfloat16):
    entries = scale * jax.random.normal(key, extent, jnp.float32)
    if shards:
        entries = entries * steps_of(key, extent, shards, -0.22, 0.18)
    return jnp.clip(with_spikes(entries, jax.random.fold_in(key, 3), *heavy), -reach, reach).astype(held_as)


def setup_inputs(seed: int = 0) -> dict:
    splits = jax.random.split(jax.random.key(seed), 7)
    return {
        "normed": noise_with(splits[0], (SEQUENCE_COUNT, SEQUENCE_LENGTH, D), 1.0, 6.0, ((0, 16), (1, 16)), (1, 2, 16, 2.0)),
        "queries": draw_queries(jax.random.fold_in(splits[6], 71), 0),
        "keys": draw_keys(jax.random.fold_in(splits[6], 71), 0),
        "values": gaussian(splits[3], (SEQUENCE_COUNT, SEQUENCE_LENGTH, KEY_VALUE_HEADS * HEAD_SIZE), 1.0, 6.0, ((0, 16), (1, 16))),
        "out_grad": gaussian(splits[4], (SEQUENCE_COUNT, SEQUENCE_LENGTH, QUERY_HEADS * HEAD_SIZE), 24.0, 150.0, ((0, 16), (1, 16))),
        "segment_ids": jax.vmap(lambda own: jnp.searchsorted(jnp.cumsum(uneven_parts(own, DOCS, SEQUENCE_LENGTH, 3 * SEQUENCE_LENGTH // 4, 1)), jnp.arange(SEQUENCE_LENGTH), side="right"))(jax.random.split(splits[5], SEQUENCE_COUNT)).reshape((SEQUENCE_COUNT, SEQUENCE_LENGTH)).astype(jnp.int32),
    }


query_scalar = 168.0


def band_core(queries, keys, values, out_grad, allowed):
    count = queries.shape[0]
    span = keys.shape[0]
    groups = keys.shape[1] // HEAD_SIZE
    ratio = queries.shape[1] // keys.shape[1]
    softmax_scale = query_scalar ** -0.5
    matmul_precision_mode = lax.Precision.HIGHEST
    query_head_rows = queries.reshape(count, groups, ratio, HEAD_SIZE).astype(jnp.float32)
    key_head_rows = keys.reshape(span, groups, HEAD_SIZE).astype(jnp.float32)
    value_head_rows = values.reshape(span, groups, HEAD_SIZE).astype(jnp.float32)
    head_gradient = out_grad.reshape(count, groups, ratio, HEAD_SIZE).astype(jnp.float32)
    attention_scores = jnp.einsum("qczw,jcw->czqj", query_head_rows, key_head_rows, precision=matmul_precision_mode) * softmax_scale
    attention_scores = jnp.where(allowed[None, None], attention_scores, -jnp.inf)
    highest = jnp.max(attention_scores, axis=-1, keepdims=True)
    expanded = jnp.exp(attention_scores - highest)
    weights_full = expanded / jnp.sum(expanded, axis=-1, keepdims=True)
    reduced_precision_weight = weights_full.astype(jnp.bfloat16).astype(jnp.float32)
    attention_output = jnp.einsum("mlhv,vmo->mlho", reduced_precision_weight, value_head_rows, precision=matmul_precision_mode)
    grad_major = jnp.transpose(head_gradient, (1, 2, 0, 3))
    delta = jnp.sum(grad_major * attention_output, axis=-1, keepdims=True)
    probability_gradient = jnp.einsum("qczw,jcw->czqj", head_gradient, value_head_rows, precision=matmul_precision_mode)
    score_gradient = (weights_full * (probability_gradient - delta)).astype(jnp.bfloat16).astype(jnp.float32)
    query_gradient = jnp.einsum("fwcj,jfe->cfwe", score_gradient, key_head_rows, precision=matmul_precision_mode) * softmax_scale
    key_gradient = jnp.einsum("vbzp,zvba->pva", score_gradient, query_head_rows, precision=matmul_precision_mode) * softmax_scale
    value_gradient = jnp.einsum("vbzp,zvba->pva", reduced_precision_weight, head_gradient, precision=matmul_precision_mode)
    return (query_gradient.reshape(count, -1).astype(jnp.bfloat16),
            key_gradient.reshape(span, -1).astype(jnp.bfloat16),
            value_gradient.reshape(span, -1).astype(jnp.bfloat16))


def one_sequence(inputs):
    queries, keys, values, out_grad, segment_ids = inputs
    width = keys.shape[1]
    span = WINDOW + TOK_DEV
    key_pad = jnp.concatenate([jnp.zeros((WINDOW, width), keys.dtype), keys], axis=0)
    value_pad = jnp.concatenate([jnp.zeros((WINDOW, width), values.dtype), values], axis=0)
    id_pad = jnp.concatenate([jnp.full((WINDOW,), -1, jnp.int32), segment_ids.astype(jnp.int32)])
    offsets = jnp.arange(TOK_DEV, dtype=jnp.int32)[:, None] - jnp.arange(span, dtype=jnp.int32)[None, :] + WINDOW

    def step(carry, index):
        key_total, value_total = carry
        start = (index * TOK_DEV).astype(jnp.int32)
        query_block = lax.dynamic_slice_in_dim(queries, start, TOK_DEV, 0)
        grad_block = lax.dynamic_slice_in_dim(out_grad, start, TOK_DEV, 0)
        key_block = lax.dynamic_slice_in_dim(key_pad, start, span, 0)
        value_block = lax.dynamic_slice_in_dim(value_pad, start, span, 0)
        query_ids = lax.dynamic_slice_in_dim(segment_ids.astype(jnp.int32), start, TOK_DEV, 0)
        key_ids = lax.dynamic_slice_in_dim(id_pad, start, span, 0)
        allowed = (query_ids[:, None] == key_ids[None, :]) & (offsets >= 0) & (offsets < WINDOW)
        query_gradient, key_gradient, value_gradient = band_core(query_block, key_block, value_block, grad_block, allowed)
        key_total = lax.dynamic_update_slice_in_dim(
            key_total, lax.dynamic_slice_in_dim(key_total, start, span, 0) + key_gradient.astype(jnp.float32), start, 0)
        value_total = lax.dynamic_update_slice_in_dim(
            value_total, lax.dynamic_slice_in_dim(value_total, start, span, 0) + value_gradient.astype(jnp.float32), start, 0)
        return (key_total, value_total), query_gradient

    zero_filled = jnp.zeros((WINDOW + SEQUENCE_LENGTH, width), jnp.float32)
    (key_total, value_total), query_gradient = lax.scan(step, (zero_filled, zero_filled), jnp.arange(N_CTX, dtype=jnp.int32))
    return (query_gradient.reshape(SEQUENCE_LENGTH, -1),
            key_total[WINDOW:].astype(jnp.bfloat16),
            value_total[WINDOW:].astype(jnp.bfloat16))


def reference(normed, queries, keys, values, out_grad, segment_ids):
    grad_queries, grad_keys, grad_values = lax.map(one_sequence, (queries, keys, values, out_grad, segment_ids))

    def sequence_step(total, pair):
        normed_seq, value_seq = pair
        input_blocks = normed_seq.reshape(N_CTX, TOK_DEV, -1)
        value_blocks = value_seq.reshape(N_CTX, TOK_DEV, -1)

        def block_step(running, block):
            term = jnp.dot(block[0].T, block[1], preferred_element_type=jnp.float32)
            return running + term.astype(jnp.bfloat16).astype(jnp.float32), None

        sequence_total, ignored = lax.scan(block_step, jnp.zeros_like(total), (input_blocks, value_blocks))
        return total + sequence_total.astype(jnp.bfloat16).astype(jnp.float32), None

    initial = jnp.zeros((normed.shape[2], values.shape[2]), jnp.float32)
    total, ignored = lax.scan(sequence_step, initial, (normed, grad_values))
    grad_weight = (total * (ALL_TOK ** -0.5)).astype(jnp.bfloat16)
    return grad_queries, grad_keys, grad_values, grad_weight
```

```python
import functools
import math

import jax
import jax.numpy as jnp
from jax import lax
from jax.experimental import pallas as pl
from jax.experimental.pallas import tpu as pltpu
from jax.sharding import Mesh, PartitionSpec as P

HEAD = 128
WINDOW = 1024
QUERY_SCALAR = 168.0
BF = jnp.bfloat16
F32 = jnp.float32
RING = 8
HOPS = (0, 4, 3, -3, 2, -2, 1, -1)


VMEM = pl.BlockSpec(memory_space=pltpu.VMEM)
SMEM = pl.BlockSpec(memory_space=pltpu.SMEM)


def call(kernel, outs, n_in, scratch=(), flops=1_000_000, name=None):
    return pl.pallas_call(
        kernel,
        out_shape=outs,
        in_specs=[SMEM] + [VMEM] * n_in,
        out_specs=jax.tree.map(lambda _: VMEM, outs),
        scratch_shapes=list(scratch),
        cost_estimate=pl.CostEstimate(flops=flops, bytes_accessed=2_000_000, transcendentals=0),
        compiler_params=pltpu.CompilerParams(vmem_limit_bytes=60_000_000),
        name=name,
    )


def shape(*dims, dtype=BF):
    return jax.ShapeDtypeStruct(dims, dtype)


def rotate(x, by):
    return lax.ppermute(x, "z", [(i, (i + by) % RING) for i in range(RING)])


def nt(a, b):
    return lax.dot_general(a, b, (((1,), (1,)), ((), ())), preferred_element_type=F32)


def nn(a, b):
    return lax.dot_general(a, b, (((1,), (0,)), ((), ())), preferred_element_type=F32)


def pack_kernel(z_ref, q, g, k, v, *outs):
    z = z_ref[0]
    for n, hop in enumerate(HOPS):
        head = lax.rem(z + hop + RING, RING)
        narrow = pl.ds(pl.multiple_of(head * HEAD, HEAD), HEAD)
        wide = pl.ds(pl.multiple_of(head * 2 * HEAD, 2 * HEAD), 2 * HEAD)
        outs[n][:, :HEAD] = k[:, narrow]
        outs[n][:, HEAD:] = v[:, narrow]
        outs[8 + n][:, : 2 * HEAD] = q[:, wide]
        outs[8 + n][:, 2 * HEAD :] = g[:, wide]


def order_kernel(z_ref, *refs):
    z = z_ref[0]
    out = refs[-1]
    rows = refs[0].shape[0]
    for ref, hop in zip(refs[:-1], HOPS):
        source = lax.rem(z - hop + RING, RING)
        out[pl.ds(pl.multiple_of(source * rows, rows), rows), :] = ref[...]


def turn_kernel(z_ref, x, out):
    tokens, features = x.shape
    part = out.shape[2]
    for b in range(features // 128):
        t = x[:, 128 * b : 128 * b + 128].T
        at = 128 * b
        while at < 128 * b + 128:
            owner = at // part
            stop = min(128 * b + 128, (owner + 1) * part)
            lo = at - owner * part
            out[owner % RING, owner // RING, lo : lo + stop - at, :] = t[at - 128 * b : stop - 128 * b]
            at = stop


def scores(kw, q, lo, scale):
    s = nt(kw, q)
    key = lax.broadcasted_iota(jnp.int32, s.shape, 0)
    row = lax.broadcasted_iota(jnp.int32, (1, s.shape[1]), 1)
    last = jnp.where(row >= 128, row - 128, row) + WINDOW
    ok = (key >= lo) & (key <= last)
    return jnp.where(ok, s * scale, -jnp.inf)


def stacked(qg, block, first):
    rows = pl.ds(pl.multiple_of(block * 128, 128), 128)
    return jnp.concatenate([qg[rows, first : first + 128], qg[rows, first + 128 : first + 256]], axis=0)


def first_kernel(scale, z_ref, lo_ref, *refs):
    pieces, (kv_own, kv_prev), (dv_prev, dv_own, stats, qg) = refs[:8], refs[8:10], refs[10:14]
    acc, keys = refs[14:]
    order_kernel(z_ref, *pieces, qg)
    acc[...] = jnp.zeros_like(acc)
    keys[:WINDOW, :] = kv_prev[:, :HEAD]
    keys[WINDOW:, :] = kv_own[:, :HEAD]

    def step(i, carry):
        span = pl.ds(pl.multiple_of(i * 128, 128), WINDOW + 128)
        lo = lo_ref[pl.ds(i, 1), :]
        s = scores(keys[span, :], stacked(qg, i, 0), lo, scale)
        top = jnp.max(s, axis=0, keepdims=True)
        e = jnp.exp2(s - top)
        inverse = 1.0 / jnp.sum(e, axis=0, keepdims=True)
        stats[pl.ds(i, 1), :] = top
        stats[pl.ds(8 + i, 1), :] = inverse
        low = (e * inverse).astype(BF)
        acc[span, :] += nn(low, stacked(qg, i, 256))
        return carry

    lax.fori_loop(0, 8, step, 0)
    dv_prev[...] = acc[:WINDOW, :].astype(BF)
    dv_own[...] = acc[WINDOW:, :]


def second_kernel(scale, softmax_scale, z_ref, lo_ref, qg, stats, kv_own, kv_prev, dk_prev, dk_own, dq, acc, keys, vals, turned):
    acc[...] = jnp.zeros_like(acc)
    keys[:WINDOW, :] = kv_prev[:, :HEAD]
    keys[WINDOW:, :] = kv_own[:, :HEAD]
    vals[:WINDOW, :] = kv_prev[:, HEAD:]
    vals[WINDOW:, :] = kv_own[:, HEAD:]
    for b in range(16):
        turned[:, 128 * b : 128 * b + 128] = keys[128 * b : 128 * b + 128, :].T

    def step(i, carry):
        at = pl.multiple_of(i * 128, 128)
        span = pl.ds(at, WINDOW + 128)
        lo = lo_ref[pl.ds(i, 1), :]
        q = stacked(qg, i, 0)
        s = scores(keys[span, :], q, lo, scale)
        full = jnp.exp2(s - stats[pl.ds(i, 1), :]) * stats[pl.ds(8 + i, 1), :]
        gp = nt(vals[span, :], stacked(qg, i, 256))
        delta = jnp.sum(full.astype(BF).astype(F32) * gp, axis=0, keepdims=True)
        ds = (full * (gp - delta)).astype(BF)
        acc[span, :] += nn(ds, q)
        back = nn(turned[:, span], ds) * softmax_scale
        dq[i, :, :HEAD] = back[:, :128].T.astype(BF)
        dq[i, :, HEAD:] = back[:, 128:].T.astype(BF)
        return carry

    lax.fori_loop(0, 8, step, 0)
    dk_prev[...] = (acc[:WINDOW, :] * softmax_scale).astype(BF)
    dk_own[...] = acc[WINDOW:, :] * softmax_scale


def weight_kernel(z_ref, features, *refs):
    blocks, (gv, mine, other), lhs = refs[:8], refs[8:11], refs[11]
    z = z_ref[0]
    core = z_ref[1]
    part = features.shape[2]
    for source in range(RING):
        for row in range(2):
            lhs[row * part : (row + 1) * part, 128 * source : 128 * source + 128] = features[source, row]
    lane = lax.broadcasted_iota(jnp.int32, (part // 2, 128), 1) < 64
    own = pl.ds(pl.multiple_of(z * 128, 128), 128)
    for ref, hop in zip(blocks, HOPS):
        head = lax.rem(z - hop + RING, RING)
        gv[:, pl.ds(pl.multiple_of(head * HEAD, HEAD), HEAD)] = ref[own, :]
        w = nn(lhs[...], ref[...])
        swapped = pltpu.roll(w, 64, 1)
        near = jnp.where(core == 0, w, swapped)
        far = jnp.where(core == 0, swapped, w)
        for row in range(2):
            a, b = row * part, row * part + part // 2
            c = b + part // 2
            mine[head, row] = jnp.where(lane, near[a:b], far[b:c])
            other[head, row] = jnp.where(lane, far[a:b], near[b:c]).astype(BF)


def body(normed, queries, keys, values, out_grad, segment_ids):
    z = lax.axis_index("z")
    yl = lax.axis_index("yl")
    core = lax.axis_index("core")
    place = jnp.stack([z, core]).astype(jnp.int32)
    softmax_scale = QUERY_SCALAR ** (-0.5)
    scale = softmax_scale * math.log2(math.e)
    count = queries.shape[1]
    features = normed.shape[2]
    part = features // 16
    row = RING * count

    packed = call(
        pack_kernel, [shape(count, 2 * HEAD)] * 8 + [shape(count, 4 * HEAD)] * 8, 4, name="pack"
    )(place, queries[0], out_grad[0], keys[0], values[0])
    kv = [packed[0]] + [rotate(packed[n], HOPS[n]) for n in range(1, 8)]
    qg = [packed[8]] + [rotate(packed[8 + n], HOPS[n]) for n in range(1, 8)]

    starts = [jnp.sum((segment_ids[0] < d).astype(jnp.int32)) for d in range(1, 4)]
    ids = lax.dynamic_slice_in_dim(segment_ids[0], yl * row, row, 0)
    doc = jnp.zeros((row,), jnp.int32)
    for d in range(1, 4):
        doc = jnp.where(ids >= d, starts[d - 1], doc)
    at = jnp.arange(row, dtype=jnp.int32)
    lo = jnp.maximum(doc - (yl * row - WINDOW + (at // count) * count), at % count + 1)
    lo = lo.reshape(RING, count)
    lo = jnp.concatenate([lo, lo], axis=1)

    turned = call(turn_kernel, shape(RING, 2, part, count), 1, name="turn")(place, normed[0])
    kv_own = call(order_kernel, shape(row, 2 * HEAD), 8, name="order")(place, *kv)
    kv_prev = lax.ppermute(kv_own, "yl", [(0, 1)])

    dv_prev, dv_own, stats, rows = call(
        functools.partial(first_kernel, scale),
        [shape(row, HEAD), shape(row, HEAD, dtype=F32), shape(16, 256, dtype=F32), shape(row, 4 * HEAD)],
        11,
        [pltpu.VMEM((2 * row, HEAD), F32), pltpu.VMEM((2 * row, HEAD), BF)],
        flops=2_000_000_000,
        name="first",
    )(place, lo, *qg, kv_own, kv_prev)
    turned, _ = lax.optimization_barrier((turned, qg[1:]))
    spread = lax.all_to_all(turned, "z", 0, 0, tiled=True)

    got = lax.ppermute(dv_prev, "yl", [(1, 0)])
    dv = (dv_own + got.astype(F32)).astype(BF)
    blocks = {0: dv}
    for s in range(1, 5):
        blocks[s] = rotate(blocks[s - 1], 1)
        if s < 4:
            blocks[-s] = rotate(blocks[1 - s], -1)

    dk_prev, dk_own, dq = call(
        functools.partial(second_kernel, scale, softmax_scale),
        [shape(row, HEAD), shape(row, HEAD, dtype=F32), shape(RING, count, 2 * HEAD)],
        5,
        [
            pltpu.VMEM((2 * row, HEAD), F32),
            pltpu.VMEM((2 * row, HEAD), BF),
            pltpu.VMEM((2 * row, HEAD), BF),
            pltpu.VMEM((HEAD, 2 * row), BF),
        ],
        flops=4_000_000_000,
        name="second",
    )(place, lo, rows, stats, kv_own, kv_prev)
    got = lax.ppermute(dk_prev, "yl", [(1, 0)])
    dk = (dk_own + got.astype(F32)).astype(BF).reshape(RING, count, HEAD)
    back = lax.all_to_all(jnp.concatenate([dq, dk], axis=2), "z", 0, 0, tiled=True)
    grad_queries = jnp.moveaxis(back[:, :, : 2 * HEAD], 0, 1).reshape(1, count, -1)
    grad_keys = jnp.moveaxis(back[:, :, 2 * HEAD :], 0, 1).reshape(1, count, -1)

    half = part // 2
    gv, mine, other = call(
        weight_kernel,
        [shape(count, RING * HEAD), shape(RING, 2, half, HEAD, dtype=F32), shape(RING, 2, half, HEAD)],
        9,
        [pltpu.VMEM((2 * part, row), BF)],
        flops=3_000_000_000,
        name="weight",
    )(place, spread, *[blocks[h] for h in HOPS])
    got = lax.ppermute(other, "core", [(0, 1), (1, 0)])
    both = (mine + got.astype(F32)).astype(BF).reshape(2 * RING, half, HEAD)
    arrived = lax.all_to_all(both, ("x", "yh", "yl"), 0, 0, tiled=True)
    total = arrived.astype(F32).sum(axis=0) * (row * 2 * 16) ** (-0.5)
    grad_weight = jnp.concatenate([total[:, :64], total[:, 64:]], axis=0).astype(BF)
    return grad_queries, grad_keys, gv[None], grad_weight


def solution(mesh):
    fine = Mesh(mesh.devices.reshape(4, 2, 2, 2, RING), ("x", "yh", "core", "yl", "z"))
    dp, ctx = ("x", "yh", "core"), ("yl", "z")
    return jax.shard_map(
        body,
        mesh=fine,
        in_specs=(P(dp, ctx, None),) * 5 + (P(dp, None),),
        out_specs=(P(dp, ctx, None),) * 3 + (P(ctx, dp),),
        check_vma=False,
    )
```

```python
import functools
import math

import jax
import jax.numpy as jnp
from jax import lax
from jax.experimental import pallas as pl
from jax.experimental.pallas import tpu as pltpu
from jax.sharding import Mesh, PartitionSpec as P


HEAD = 128
WINDOW = 1024
QUERY_SCALAR = 168.0
BF = jnp.bfloat16
F32 = jnp.float32
RING = 8
HOPS = (0, 4, 3, -3, 2, -2, 1, -1)
PARTS = ((0, 4), (4, 8))


VMEM = pl.BlockSpec(memory_space=pltpu.VMEM)
SMEM = pl.BlockSpec(memory_space=pltpu.SMEM)


def call(kernel, outs, n_in, scratch=(), flops=1_000_000):
    return pl.pallas_call(
        kernel,
        out_shape=outs,
        in_specs=[SMEM] + [VMEM] * n_in,
        out_specs=jax.tree.map(lambda _: VMEM, outs),
        scratch_shapes=list(scratch),
        cost_estimate=pl.CostEstimate(flops=flops, bytes_accessed=2_000_000, transcendentals=0),
        compiler_params=pltpu.CompilerParams(vmem_limit_bytes=60_000_000),
    )


def shape(*dims, dtype=BF):
    return jax.ShapeDtypeStruct(dims, dtype)


def rotate(x, by):
    return lax.ppermute(x, "z", [(i, (i + by) % RING) for i in range(RING)])


def nt(a, b):
    return lax.dot_general(a, b, (((1,), (1,)), ((), ())), preferred_element_type=F32)


def nn(a, b):
    return lax.dot_general(a, b, (((1,), (0,)), ((), ())), preferred_element_type=F32)


def heads_kernel(z_ref, k, v, kv):
    for head in range(RING):
        kv[head, :, :HEAD] = k[:, head * HEAD : (head + 1) * HEAD]
        kv[head, :, HEAD:] = v[:, head * HEAD : (head + 1) * HEAD]


def pack_kernel(z_ref, q, g, *outs):
    z = z_ref[0]
    for n, hop in enumerate(HOPS):
        head = lax.rem(z + hop + RING, RING)
        wide = pl.ds(pl.multiple_of(head * 2 * HEAD, 2 * HEAD), 2 * HEAD)
        outs[n][:, : 2 * HEAD] = q[:, wide]
        outs[n][:, 2 * HEAD :] = g[:, wide]


def in_order(z, pieces, out):
    rows = pieces[0].shape[0]
    for ref, hop in zip(pieces, HOPS):
        source = lax.rem(z - hop + RING, RING)
        out[pl.ds(pl.multiple_of(source * rows, rows), rows), :] = ref[...]


def turn_kernel(z_ref, ids, x, out, lo_ref):
    _, features = x.shape
    part = out.shape[2]
    for b in range(features // 128):
        t = x[:, 128 * b : 128 * b + 128].T
        at = 128 * b
        while at < 128 * b + 128:
            owner = at // part
            stop = min(128 * b + 128, (owner + 1) * part)
            lo = at - owner * part
            out[owner % RING, owner // RING, lo : lo + stop - at, :] = t[at - 128 * b : stop - 128 * b]
            at = stop
    yl = z_ref[2]
    every = ids[...]
    own = ids[pl.ds(pl.multiple_of(yl * RING, RING), RING), :]
    doc = jnp.zeros(own.shape, jnp.int32)
    for d in range(1, 4):
        doc = jnp.where(own >= d, jnp.sum((every < d).astype(jnp.int32)), doc)
    block = lax.broadcasted_iota(jnp.int32, own.shape, 0)
    at = lax.broadcasted_iota(jnp.int32, own.shape, 1)
    lo = jnp.maximum(doc - (yl * (RING * 128) - WINDOW + block * 128), at + 1)
    lo_ref[:, :128] = lo
    lo_ref[:, 128:] = lo


def scores(kw, q, lo, scale):
    s = nt(kw, q)
    key = lax.broadcasted_iota(jnp.int32, s.shape, 0)
    row = lax.broadcasted_iota(jnp.int32, (1, s.shape[1]), 1)
    last = jnp.where(row >= 128, row - 128, row) + WINDOW
    ok = (key >= lo) & (key <= last)
    return jnp.where(ok, s * scale, -jnp.inf)


def stacked(qg, block, first):
    rows = pl.ds(pl.multiple_of(block * 128, 128), 128)
    return jnp.concatenate([qg[rows, first : first + 128], qg[rows, first + 128 : first + 256]], axis=0)


def first_kernel(scale, z_ref, lo_ref, *refs):
    pieces, (kv_own, kv_prev), (dv_prev, dv_own, stats, qg) = refs[:8], refs[8:10], refs[10:14]
    acc, keys = refs[14:]
    in_order(z_ref[0], pieces, qg)
    acc[...] = jnp.zeros_like(acc)
    keys[:WINDOW, :] = kv_prev[:, :HEAD]
    keys[WINDOW:, :] = kv_own[:, :HEAD]

    def step(i, carry):
        span = pl.ds(pl.multiple_of(i * 128, 128), WINDOW + 128)
        lo = lo_ref[pl.ds(i, 1), :]
        s = scores(keys[span, :], stacked(qg, i, 0), lo, scale)
        top = jnp.max(s, axis=0, keepdims=True)
        e = jnp.exp2(s - top)
        inverse = 1.0 / jnp.sum(e, axis=0, keepdims=True)
        stats[pl.ds(i, 1), :] = top
        stats[pl.ds(8 + i, 1), :] = inverse
        low = (e * inverse).astype(BF)
        acc[span, :] += nn(low, stacked(qg, i, 256))
        return carry

    lax.fori_loop(0, 8, step, 0, unroll=True)
    dv_prev[...] = acc[:WINDOW, :].astype(BF)
    dv_own[...] = acc[WINDOW:, :]


def second_kernel(scale, softmax_scale, lower, upper, z_ref, lo_ref, qg, stats, kv_own, kv_prev, *refs):
    acc, dq = refs[1:3] if lower else refs[:2]
    dk_prev, keys, vals, turned = refs[-4:]
    acc[...] = refs[0][...] if lower else jnp.zeros_like(acc)
    begin, end = 128 * lower, 128 * upper
    keys[begin:WINDOW, :] = kv_prev[begin:, :HEAD]
    keys[WINDOW : WINDOW + end, :] = kv_own[:end, :HEAD]
    vals[begin:WINDOW, :] = kv_prev[begin:, HEAD:]
    vals[WINDOW : WINDOW + end, :] = kv_own[:end, HEAD:]
    for b in range(lower, upper + 8):
        turned[:, 128 * b : 128 * b + 128] = keys[128 * b : 128 * b + 128, :].T

    def step(i, carry):
        at = pl.multiple_of(i * 128, 128)
        span = pl.ds(at, WINDOW + 128)
        lo = lo_ref[pl.ds(i, 1), :]
        q = stacked(qg, i, 0)
        s = scores(keys[span, :], q, lo, scale)
        full = jnp.exp2(s - stats[pl.ds(i, 1), :]) * stats[pl.ds(8 + i, 1), :]
        gp = nt(vals[span, :], stacked(qg, i, 256))
        delta = jnp.sum(full.astype(BF).astype(F32) * gp, axis=0, keepdims=True)
        ds = (full * (gp - delta)).astype(BF)
        acc[span, :] += nn(ds, q)
        back = nn(turned[:, span], ds) * softmax_scale
        dq[i - lower, :, :HEAD] = back[:, :128].T.astype(BF)
        dq[i - lower, :, HEAD:] = back[:, 128:].T.astype(BF)
        return carry

    lax.fori_loop(lower, upper, step, 0, unroll=True)
    if upper == RING:
        dk_prev[...] = (acc[:WINDOW, :] * softmax_scale).astype(BF)


def back_kernel(softmax_scale, z_ref, low, high, acc, got, *outs):
    z = z_ref[0]
    split = low.shape[0]
    for n, hop in enumerate(HOPS):
        block = lax.rem(z + hop + RING, RING)
        rows = pl.ds(pl.multiple_of(block * HEAD, HEAD), HEAD)
        upper = pl.ds(pl.multiple_of(WINDOW + block * HEAD, HEAD), HEAD)

        @pl.when(block < split)
        def _():
            outs[n][:, : 2 * HEAD] = low[jnp.minimum(block, split - 1)]

        @pl.when(block >= split)
        def _():
            outs[n][:, : 2 * HEAD] = high[jnp.maximum(block - split, 0)]

        outs[n][:, 2 * HEAD :] = (acc[upper, :] * softmax_scale + got[rows, :].astype(F32)).astype(BF)


def unpack_kernel(z_ref, *refs):
    z = z_ref[0]
    dq, dk = refs[-2:]
    for ref, hop in zip(refs[:-2], HOPS):
        head = lax.rem(z - hop + RING, RING)
        dq[:, pl.ds(pl.multiple_of(head * 2 * HEAD, 2 * HEAD), 2 * HEAD)] = ref[:, : 2 * HEAD]
        dk[:, pl.ds(pl.multiple_of(head * HEAD, HEAD), HEAD)] = ref[:, 2 * HEAD :]


def halves(w, core, part):
    lane = lax.broadcasted_iota(jnp.int32, (part // 2, 128), 1) < 64
    swapped = pltpu.roll(w, 64, 1)
    near = jnp.where(core == 0, w, swapped)
    far = jnp.where(core == 0, swapped, w)
    out = []
    for row in range(2):
        a, b = row * part, row * part + part // 2
        c = b + part // 2
        out.append((jnp.where(lane, near[a:b], far[b:c]), jnp.where(lane, far[a:b], near[b:c]).astype(BF)))
    return out


def weight_kernel(hops, z_ref, features, *refs):
    n = len(hops)
    blocks, (gv, mine, other, lhs) = refs[:n], refs[n:]
    z = z_ref[0]
    part = features.shape[2]
    for source in range(RING):
        for row in range(2):
            lhs[row * part : (row + 1) * part, 128 * source : 128 * source + 128] = features[source, row]
    own = pl.ds(pl.multiple_of(z * 128, 128), 128)
    for ref, hop in zip(blocks, hops):
        head = lax.rem(z - hop + RING, RING)
        gv[:, pl.ds(pl.multiple_of(head * HEAD, HEAD), HEAD)] = ref[own, :]
        for row, (a, b) in enumerate(halves(nn(lhs[...], ref[...]), z_ref[1], part)):
            mine[head, row] = a
            other[head, row] = b


def last_weight_kernel(z_ref, lhs, block, mine, other):
    part = lhs.shape[0] // 2
    for row, (a, b) in enumerate(halves(nn(lhs[...], block[...]), z_ref[1], part)):
        mine[row] = a
        other[row] = b


def join_kernel(z_ref, both, last, got, out, total, sem):
    total[...] = (last[...] + got[...].astype(F32)).astype(BF)
    copy = pltpu.make_async_copy(total, out.at[lax.rem(z_ref[0] + 4, RING)], sem)
    copy.start()
    copy.wait()


def body(normed, queries, keys, values, out_grad, segment_ids):
    z = lax.axis_index("z")
    yl = lax.axis_index("yl")
    core = lax.axis_index("core")
    place = jnp.stack([z, core, yl]).astype(jnp.int32)
    softmax_scale = QUERY_SCALAR ** (-0.5)
    scale = softmax_scale * math.log2(math.e)
    count = queries.shape[1]
    features = normed.shape[2]
    part = features // 16
    half = part // 2
    row = RING * count

    packed = call(heads_kernel, shape(RING, count, 2 * HEAD), 2)(place, keys[0], values[0])
    kv_own = lax.all_to_all(packed, "z", 0, 0, tiled=True).reshape(row, 2 * HEAD)
    packed = call(pack_kernel, [shape(count, 4 * HEAD)] * 8, 2)(place, queries[0], out_grad[0])
    qg = [packed[0]]
    for n in range(1, 8):
        qg.append(rotate(packed[n], HOPS[n]))
    turned, lo = call(
        turn_kernel, [shape(RING, 2, part, count), shape(RING, 256, dtype=jnp.int32)], 2
    )(place, segment_ids.reshape(2 * RING, count), normed[0])
    kv_prev = lax.ppermute(kv_own, "yl", [(0, 1)])
    spread = lax.all_to_all(turned, "z", 0, 0, tiled=True)

    dv_prev, dv_own, stats, rows = call(
        functools.partial(first_kernel, scale),
        [shape(row, HEAD), shape(row, HEAD, dtype=F32), shape(16, 256, dtype=F32), shape(row, 4 * HEAD)],
        11,
        [pltpu.VMEM((2 * row, HEAD), F32), pltpu.VMEM((2 * row, HEAD), BF)],
        flops=2_000_000_000,
    )(place, lo, *qg, kv_own, kv_prev)

    got = lax.ppermute(dv_prev, "yl", [(1, 0)])
    dv = (dv_own + got.astype(F32)).astype(BF)
    blocks = {0: dv}
    for s in range(1, 5):
        blocks[s] = rotate(blocks[s - 1], 1)
        if s < 4:
            blocks[-s] = rotate(blocks[1 - s], -1)

    acc = None
    dq = []
    for n, (lower, upper) in enumerate(PARTS):
        outs = [shape(2 * row, HEAD, dtype=F32), shape(upper - lower, count, 2 * HEAD), shape(row, HEAD)]
        acc, piece, dk_prev = call(
            functools.partial(second_kernel, scale, softmax_scale, lower, upper),
            outs,
            5 + (n > 0),
            [pltpu.VMEM((2 * row, HEAD), BF), pltpu.VMEM((2 * row, HEAD), BF), pltpu.VMEM((HEAD, 2 * row), BF)],
            flops=1_500_000_000,
        )(place, lo, rows, stats, kv_own, kv_prev, *([acc] if n else []))
        dq.append(piece)
    got = lax.ppermute(dk_prev, "yl", [(1, 0)])
    back = call(functools.partial(back_kernel, softmax_scale), [shape(count, 3 * HEAD)] * 8, 4)(place, *dq, acc, got)
    home = [back[0]]
    for n in range(1, 8):
        home.append(rotate(back[n], HOPS[n]))
    grad_queries, grad_keys = call(
        unpack_kernel, [shape(count, 2 * RING * HEAD), shape(count, RING * HEAD)], 8
    )(place, *home)

    early = [h for h in HOPS if h != 4]
    gv, mine, other, lhs = call(
        functools.partial(weight_kernel, early),
        [
            shape(count, RING * HEAD),
            shape(RING, 2, half, HEAD, dtype=F32),
            shape(RING, 2, half, HEAD),
            shape(2 * part, row),
        ],
        8,
        flops=2_000_000_000,
    )(place, spread, *[blocks[h] for h in early])
    got = lax.ppermute(other, "core", [(0, 1), (1, 0)])
    both = (mine + got.astype(F32)).astype(BF)
    last, other = call(
        last_weight_kernel, [shape(2, half, HEAD, dtype=F32), shape(2, half, HEAD)], 2, flops=300_000_000
    )(place, lhs, blocks[4])
    got = lax.ppermute(other, "core", [(0, 1), (1, 0)])
    both = pl.pallas_call(
        join_kernel,
        out_shape=shape(RING, 2, half, HEAD),
        in_specs=[SMEM, pl.BlockSpec(memory_space=pl.ANY), VMEM, VMEM],
        out_specs=pl.BlockSpec(memory_space=pl.ANY),
        scratch_shapes=[pltpu.VMEM((2, half, HEAD), BF), pltpu.SemaphoreType.DMA],
        input_output_aliases={1: 0},
        name="join",
    )(place, both, last, got)
    arrived = lax.all_to_all(both.reshape(2 * RING, half, HEAD), ("x", "yh", "yl"), 0, 0, tiled=True)
    total = arrived.astype(F32).sum(axis=0) * (row * 2 * 16) ** (-0.5)
    grad_weight = jnp.concatenate([total[:, :64], total[:, 64:]], axis=0).astype(BF)
    far = lax.dynamic_slice_in_dim(blocks[4], z * count, count, 0)
    gv = lax.dynamic_update_slice_in_dim(gv, far, lax.rem(z + 4, RING) * HEAD, 1)
    return grad_queries[None], grad_keys[None], gv[None], grad_weight


def solution(mesh):
    fine = Mesh(mesh.devices.reshape(4, 2, 2, 2, RING), ("x", "yh", "core", "yl", "z"))
    dp, ctx = ("x", "yh", "core"), ("yl", "z")

    return jax.shard_map(
        body,
        mesh=fine,
        in_specs=(P(dp, ctx, None),) * 5 + (P(dp, None),),
        out_specs=(P(dp, ctx, None),) * 3 + (P(ctx, dp),),
        check_vma=False,
    )
```

```python
import functools
import math

import jax
import jax.numpy as jnp
from jax import lax
from jax.experimental import pallas as pl
from jax.experimental.pallas import tpu as pltpu
from jax.sharding import Mesh, PartitionSpec as P


HEAD = 128
WINDOW = 1024
QUERY_SCALAR = 168.0
BF = jnp.bfloat16
F32 = jnp.float32
RING = 8
HOPS = (0, 4, 3, -3, 2, -2, 1, -1)
PARTS = ((0, 4), (4, 8))
GROUPS = ((0, 1, -1), (2, -2), (3, -3), (4,))
SOON = (4, 3, -3)
LATE = (0, 2, -2, 1, -1)
LIMIT = 4_000_000
LARGE = 10_000_000


VMEM = pl.BlockSpec(memory_space=pltpu.VMEM)
ANY = pl.BlockSpec(memory_space=pl.ANY)
SMEM = pl.BlockSpec(memory_space=pltpu.SMEM)


def call(kernel, outs, n_in, scratch=(), flops=1_000_000, limit=LIMIT, loose=(), loose_out=False):
    return pl.pallas_call(
        kernel,
        out_shape=outs,
        in_specs=[SMEM] + [ANY if n in loose else VMEM for n in range(n_in)],
        out_specs=jax.tree.map(lambda _: ANY if loose_out else VMEM, outs),
        scratch_shapes=list(scratch),
        cost_estimate=pl.CostEstimate(flops=flops, bytes_accessed=2_000_000, transcendentals=0),
        compiler_params=pltpu.CompilerParams(vmem_limit_bytes=limit),
    )


def shape(*dims, dtype=BF):
    return jax.ShapeDtypeStruct(dims, dtype)


def rotate(x, by):
    return lax.ppermute(x, "z", [(i, (i + by) % RING) for i in range(RING)])


def nt(a, b):
    return lax.dot_general(a, b, (((1,), (1,)), ((), ())), preferred_element_type=F32)


def nn(a, b):
    return lax.dot_general(a, b, (((1,), (0,)), ((), ())), preferred_element_type=F32)


def heads_kernel(k, v, kv, sem):
    copies = []
    for head in range(RING):
        columns = pl.ds(head * HEAD, HEAD)
        copies.append(pltpu.make_async_copy(k.at[:, columns], kv.at[head, :, pl.ds(0, HEAD)], sem.at[head]))
        copies.append(pltpu.make_async_copy(v.at[:, columns], kv.at[head, :, pl.ds(HEAD, HEAD)], sem.at[RING + head]))
    for copy in copies:
        copy.start()
    for copy in copies:
        copy.wait()


def pack_kernel(z_ref, q, g, *outs):
    z = z_ref[0]
    for n, hop in enumerate(HOPS):
        head = lax.rem(z + hop + RING, RING)
        wide = pl.ds(pl.multiple_of(head * 2 * HEAD, 2 * HEAD), 2 * HEAD)
        outs[n][:, : 2 * HEAD] = q[:, wide]
        outs[n][:, 2 * HEAD :] = g[:, wide]


def in_order(z, pieces, out, sem):
    rows = pieces[0].shape[0]
    copies = []
    for n, (ref, hop) in enumerate(zip(pieces, HOPS)):
        source = lax.rem(z - hop + RING, RING)
        at = out.at[pl.ds(pl.multiple_of(source * rows, rows), rows), :]
        copies.append(pltpu.make_async_copy(ref, at, sem.at[n]))
        copies[-1].start()
    return copies


def turn_kernel(z_ref, ids, x, out, lo_ref):
    _, features = x.shape
    part = out.shape[2]
    for b in range(features // 128):
        t = x[:, 128 * b : 128 * b + 128].T
        at = 128 * b
        while at < 128 * b + 128:
            owner = at // part
            stop = min(128 * b + 128, (owner + 1) * part)
            lo = at - owner * part
            out[owner % RING, owner // RING, lo : lo + stop - at, :] = t[at - 128 * b : stop - 128 * b]
            at = stop
    yl = z_ref[2]
    every = ids[...]
    own = ids[pl.ds(pl.multiple_of(yl * RING, RING), RING), :]
    doc = jnp.zeros(own.shape, jnp.int32)
    for d in range(1, 4):
        doc = jnp.where(own >= d, jnp.sum((every < d).astype(jnp.int32)), doc)
    block = lax.broadcasted_iota(jnp.int32, own.shape, 0)
    at = lax.broadcasted_iota(jnp.int32, own.shape, 1)
    lo = jnp.maximum(doc - (yl * (RING * 128) - WINDOW + block * 128), at + 1)
    lo_ref[:, :128] = lo
    lo_ref[:, 128:] = lo


def scores(kw, q, lo, scale):
    s = nt(kw, q)
    key = lax.broadcasted_iota(jnp.int32, s.shape, 0)
    row = lax.broadcasted_iota(jnp.int32, (1, s.shape[1]), 1)
    last = jnp.where(row >= 128, row - 128, row) + WINDOW
    ok = (key >= lo) & (key <= last)
    return jnp.where(ok, s * scale, -jnp.inf)


def stacked(qg, block, first):
    rows = pl.ds(pl.multiple_of(block * 128, 128), 128)
    return jnp.concatenate([qg[rows, first : first + 128], qg[rows, first + 128 : first + 256]], axis=0)


def first_kernel(scale, z_ref, lo_ref, *refs):
    pieces, (kv_own, kv_prev), (dv_prev, dv_own, stats, qg) = refs[:8], refs[8:10], refs[10:14]
    acc, keys, sem = refs[14:]
    copies = in_order(z_ref[0], pieces, qg, sem)
    acc[...] = jnp.zeros_like(acc)
    keys[:WINDOW, :] = kv_prev[:, :HEAD]
    keys[WINDOW:, :] = kv_own[:, :HEAD]
    for copy in copies:
        copy.wait()

    def step(i, carry):
        span = pl.ds(pl.multiple_of(i * 128, 128), WINDOW + 128)
        lo = lo_ref[pl.ds(i, 1), :]
        s = scores(keys[span, :], stacked(qg, i, 0), lo, scale)
        top = jnp.max(s, axis=0, keepdims=True)
        e = jnp.exp2(s - top)
        inverse = 1.0 / jnp.sum(e, axis=0, keepdims=True)
        stats[pl.ds(i, 1), :] = top
        stats[pl.ds(8 + i, 1), :] = inverse
        low = (e * inverse).astype(BF)
        acc[span, :] += nn(low, stacked(qg, i, 256))
        return carry

    lax.fori_loop(0, 8, step, 0, unroll=True)
    dv_prev[...] = acc[:WINDOW, :].astype(BF)
    dv_own[...] = acc[WINDOW:, :]


def second_kernel(scale, softmax_scale, lower, upper, z_ref, lo_ref, qg, stats, kv_own, kv_prev, *refs):
    acc, dq = refs[1:3] if lower else refs[:2]
    dk_prev, keys, vals, turned = refs[-4:]
    acc[...] = refs[0][...] if lower else jnp.zeros_like(acc)
    begin, end = 128 * lower, 128 * upper
    keys[begin:WINDOW, :] = kv_prev[begin:, :HEAD]
    keys[WINDOW : WINDOW + end, :] = kv_own[:end, :HEAD]
    vals[begin:WINDOW, :] = kv_prev[begin:, HEAD:]
    vals[WINDOW : WINDOW + end, :] = kv_own[:end, HEAD:]
    for b in range(lower, upper + 8):
        turned[:, 128 * b : 128 * b + 128] = keys[128 * b : 128 * b + 128, :].T

    def step(i, carry):
        at = pl.multiple_of(i * 128, 128)
        span = pl.ds(at, WINDOW + 128)
        lo = lo_ref[pl.ds(i, 1), :]
        q = stacked(qg, i, 0)
        s = scores(keys[span, :], q, lo, scale)
        full = jnp.exp2(s - stats[pl.ds(i, 1), :]) * stats[pl.ds(8 + i, 1), :]
        gp = nt(vals[span, :], stacked(qg, i, 256))
        delta = jnp.sum(full.astype(BF).astype(F32) * gp, axis=0, keepdims=True)
        ds = (full * (gp - delta)).astype(BF)
        acc[span, :] += nn(ds, q)
        back = nn(turned[:, span], ds) * softmax_scale
        dq[i - lower, :, :HEAD] = back[:, :128].T.astype(BF)
        dq[i - lower, :, HEAD:] = back[:, 128:].T.astype(BF)
        return carry

    lax.fori_loop(lower, upper, step, 0, unroll=2)
    if upper == RING:
        dk_prev[...] = (acc[:WINDOW, :] * softmax_scale).astype(BF)


def back_kernel(softmax_scale, hops, z_ref, low, high, acc, got, *outs):
    z = z_ref[0]
    split = low.shape[0]
    for out, hop in zip(outs, hops):
        block = lax.rem(z + hop + RING, RING)
        rows = pl.ds(pl.multiple_of(block * HEAD, HEAD), HEAD)
        upper = pl.ds(pl.multiple_of(WINDOW + block * HEAD, HEAD), HEAD)

        @pl.when(block < split)
        def _():
            out[:, : 2 * HEAD] = low[jnp.minimum(block, split - 1)]

        @pl.when(block >= split)
        def _():
            out[:, : 2 * HEAD] = high[jnp.maximum(block - split, 0)]

        out[:, 2 * HEAD :] = (acc[upper, :] * softmax_scale + got[rows, :].astype(F32)).astype(BF)


def unpack_kernel(z_ref, *refs):
    z = z_ref[0]
    dq, dk, sem = refs[8:]
    copies = []
    for n, (ref, hop) in enumerate(zip(refs[:8], HOPS)):
        head = lax.rem(z - hop + RING, RING)
        wide = pl.ds(pl.multiple_of(head * 2 * HEAD, 2 * HEAD), 2 * HEAD)
        narrow = pl.ds(pl.multiple_of(head * HEAD, HEAD), HEAD)
        copies.append(pltpu.make_async_copy(ref.at[:, pl.ds(0, 2 * HEAD)], dq.at[:, wide], sem.at[n]))
        copies.append(pltpu.make_async_copy(ref.at[:, pl.ds(2 * HEAD, HEAD)], dk.at[:, narrow], sem.at[8 + n]))
    for copy in copies:
        copy.start()
    for copy in copies:
        copy.wait()


def halves(w, core, part):
    lane = lax.broadcasted_iota(jnp.int32, (part // 2, 128), 1) < 64
    swapped = pltpu.roll(w, 64, 1)
    near = jnp.where(core == 0, w, swapped)
    far = jnp.where(core == 0, swapped, w)
    out = []
    for row in range(2):
        a, b = row * part, row * part + part // 2
        c = b + part // 2
        out.append((jnp.where(lane, near[a:b], far[b:c]), jnp.where(lane, far[a:b], near[b:c]).astype(BF)))
    return out


def weight_kernel(n, z_ref, left, *refs):
    blocks, (rows, mine, other) = refs[:n], refs[n : n + 3]
    lhs = left
    if len(refs) > n + 3:
        lhs = refs[n + 3]
        part = left.shape[2]
        for source in range(RING):
            for row in range(2):
                lhs[row * part : (row + 1) * part, 128 * source : 128 * source + 128] = left[source, row]
    part = lhs.shape[0] // 2
    own = pl.ds(pl.multiple_of(z_ref[0] * 128, 128), 128)
    for m, ref in enumerate(blocks):
        rows[m] = ref[own, :]
        for row, (a, b) in enumerate(halves(nn(lhs[...], ref[...]), z_ref[1], part)):
            mine[m, row] = a
            other[m, row] = b


def join_kernel(z_ref, *refs):
    out = refs[-1]
    for n, hops in enumerate(GROUPS):
        for m, hop in enumerate(hops):
            head = lax.rem(z_ref[0] - hop + RING, RING)
            out[head] = (refs[2 * n][m] + refs[2 * n + 1][m].astype(F32)).astype(BF)


def values_kernel(z_ref, *refs):
    out = refs[-1]
    for ref, hops in zip(refs[:-1], GROUPS):
        for m, hop in enumerate(hops):
            head = lax.rem(z_ref[0] - hop + RING, RING)
            out[:, pl.ds(pl.multiple_of(head * HEAD, HEAD), HEAD)] = ref[m]


def body(normed, queries, keys, values, out_grad, segment_ids):
    z = lax.axis_index("z")
    yl = lax.axis_index("yl")
    core = lax.axis_index("core")
    place = jnp.stack([z, core, yl]).astype(jnp.int32)
    softmax_scale = QUERY_SCALAR ** (-0.5)
    scale = softmax_scale * math.log2(math.e)
    count = queries.shape[1]
    features = normed.shape[2]
    part = features // 16
    half = part // 2
    row = RING * count

    packed = pl.pallas_call(
        heads_kernel,
        out_shape=shape(RING, count, 2 * HEAD),
        in_specs=[pl.BlockSpec(memory_space=pl.ANY)] * 2,
        out_specs=VMEM,
        scratch_shapes=[pltpu.SemaphoreType.DMA((2 * RING,))],
        compiler_params=pltpu.CompilerParams(vmem_limit_bytes=60_000_000),
        name="heads",
    )(keys[0], values[0])
    kv_own = lax.all_to_all(packed, "z", 0, 0, tiled=True).reshape(row, 2 * HEAD)
    packed = call(pack_kernel, [shape(count, 4 * HEAD)] * 8, 2)(place, queries[0], out_grad[0])
    qg = [packed[0]]
    for n in range(1, 8):
        qg.append(rotate(packed[n], HOPS[n]))
    turned, lo = call(
        turn_kernel, [shape(RING, 2, part, count), shape(RING, 256, dtype=jnp.int32)], 2
    )(place, segment_ids.reshape(2 * RING, count), normed[0])
    kv_prev = lax.ppermute(kv_own, "yl", [(0, 1)])
    spread = lax.all_to_all(turned, "z", 0, 0, tiled=True)

    dv_prev, dv_own, stats, rows = call(
        functools.partial(first_kernel, scale),
        [shape(row, HEAD), shape(row, HEAD, dtype=F32), shape(16, 256, dtype=F32), shape(row, 4 * HEAD)],
        11,
        [pltpu.VMEM((2 * row, HEAD), F32), pltpu.VMEM((2 * row, HEAD), BF), pltpu.SemaphoreType.DMA((RING,))],
        flops=2_000_000_000,
        loose=range(1, 9),
        limit=LARGE,
    )(place, lo, *qg, kv_own, kv_prev)

    got = lax.ppermute(dv_prev, "yl", [(1, 0)])
    dv = (dv_own + got.astype(F32)).astype(BF)
    blocks = {0: dv}
    for s in range(1, 5):
        blocks[s] = rotate(blocks[s - 1], 1)
        if s < 4:
            blocks[-s] = rotate(blocks[1 - s], -1)

    acc = None
    dq = []
    for n, (lower, upper) in enumerate(PARTS):
        outs = [shape(2 * row, HEAD, dtype=F32), shape(upper - lower, count, 2 * HEAD), shape(row, HEAD)]
        acc, piece, dk_prev = call(
            functools.partial(second_kernel, scale, softmax_scale, lower, upper),
            outs,
            5 + (n > 0),
            [pltpu.VMEM((2 * row, HEAD), BF), pltpu.VMEM((2 * row, HEAD), BF), pltpu.VMEM((HEAD, 2 * row), BF)],
            flops=1_500_000_000,
            limit=LARGE,
        )(place, lo, rows, stats, kv_own, kv_prev, *([acc] if n else []))
        dq.append(piece)
    got = lax.ppermute(dk_prev, "yl", [(1, 0)])
    pieces = {}
    for hops in (SOON, LATE):
        outs = call(
            functools.partial(back_kernel, softmax_scale, hops), [shape(count, 3 * HEAD)] * len(hops), 4
        )(place, *dq, acc, got)
        pieces.update(zip(hops, outs))
    home = [pieces[0]]
    for n in range(1, 8):
        home.append(rotate(pieces[HOPS[n]], HOPS[n]))
    grad_queries, grad_keys = call(
        unpack_kernel, [shape(count, 2 * RING * HEAD), shape(count, RING * HEAD)], 8,
        [pltpu.SemaphoreType.DMA((16,))], loose=range(8),
    )(place, *home)

    left = spread
    values_own, sums = [], []
    for n, hops in enumerate(GROUPS):
        size = len(hops)
        outs = [shape(size, count, HEAD), shape(size, 2, half, HEAD, dtype=F32), shape(size, 2, half, HEAD)]
        if n == 0:
            outs.append(shape(2 * part, row))
        own_rows, mine, other, *lhs = call(
            functools.partial(weight_kernel, size), outs, 1 + size, flops=300_000_000 * size
        )(place, left, *[blocks[h] for h in hops])
        if n == 0:
            left = lhs[0]
        values_own.append(own_rows)
        sums += [mine, lax.ppermute(other, "core", [(0, 1), (1, 0)])]
    both = call(join_kernel, shape(RING, 2, half, HEAD), 8)(place, *sums)
    arrived = lax.all_to_all(both.reshape(2 * RING, half, HEAD), ("x", "yh", "yl"), 0, 0, tiled=True)
    total = arrived.astype(F32).sum(axis=0) * (row * 2 * 16) ** (-0.5)
    grad_weight = jnp.concatenate([total[:, :64], total[:, 64:]], axis=0).astype(BF)
    gv = call(values_kernel, shape(count, RING * HEAD), 4)(place, *values_own)
    return grad_queries[None], grad_keys[None], gv[None], grad_weight


def solution(mesh):
    fine = Mesh(mesh.devices.reshape(4, 2, 2, 2, RING), ("x", "yh", "core", "yl", "z"))
    dp, ctx = ("x", "yh", "core"), ("yl", "z")

    return jax.shard_map(
        body,
        mesh=fine,
        in_specs=(P(dp, ctx, None),) * 5 + (P(dp, None),),
        out_specs=(P(dp, ctx, None),) * 3 + (P(ctx, dp),),
        check_vma=False,
    )
```
